32 devices in a mesh: gx: 4 (over y, x), gy: 2 (over core), gz: 4 (over z).
Axes of the slice: x: 2, y: 2, z: 4, core: 2. Of those that a mesh axis runs over, the one named last changes fastest.
Arguments:
- start_block: float32 [64, 3, 8, 16, 512], P(None, None, 'gx', 'gy', 'gz'), may hold values from -6 to 6
- stiff_field: float32 [8, 16, 512], P('gx', 'gy', 'gz'), may hold values from 0.5 to 2
- shift_field: float32 [8, 16, 512], P('gx', 'gy', 'gz'), may hold values from 0.25 to 2
- mass_field: float32 [8, 16, 512], P('gx', 'gy', 'gz'), may hold values from 0.5 to 2
Outputs:
- modes: float32 [64, 3, 8, 16, 512], P(None, None, 'gx', 'gy', 'gz')
- ritz: float32 [64, 64], replicated
The draws below stay inside these ranges and needn't reach their ends.
All inputs are finite; a program needn't handle non-finite values. Where the reference program divides by a largest or mean magnitude, that divisor is 1e-20 or more.
Results may differ from the reference program's by a relative error of at most 0.0003.
Values sent between devices are 32-bit elements; how exact they have to be, the bound alone decides.
No kernel may reach another device: no remote copies, remote signals or barrier semaphores. Data moves between devices by JAX's collectives and lax.ppermute only.
A program may use at most 128 MiB of HBM per device.

```python
import math
import jax
import jax.numpy as jnp
from jax import lax

MODES = 64
ITERS = 2
FILTER = 4
NX = 8
NY = 16
NZ = 512
DOFS = 196608


def steps_of(rng, shape, cuts, smallest, top_value):
    def one(axis_at, parts):
        steps = jax.random.uniform(jax.random.fold_in(jax.random.fold_in(rng, 6), axis_at), (parts,), jnp.float32, smallest / len(cuts), top_value / len(cuts))
        return jnp.repeat(jnp.exp(steps), shape[axis_at] // parts).reshape((-1,) + (1,) * (len(shape) - axis_at - 1))

    gain = one(*cuts[0])
    for cut in cuts[1:]:
        gain = gain * one(*cut)
    return gain


def noise(key, shape, scale, limit, cuts=(), dtype=jnp.bfloat16):
    result = jax.random.normal(key, shape, jnp.float32) * scale
    if len(cuts) > 0:
        result = steps_of(key, shape, cuts, -0.22, 0.18) * result
    return jnp.clip(result, min=-limit, max=limit).astype(dtype)


def setup_inputs(seed: int = 0) -> dict:
    seeds = jax.random.split(jax.random.key(seed), 5)
    start_block = noise(seeds[0], (MODES, 3, NX, NY, NZ), 1.0, 6.0, ((2, 4), (3, 2), (4, 4)), jnp.float32)
    stiff_field = jnp.clip(jnp.exp(math.log(2.0) - 1.3862944 * jax.random.uniform(seeds[1], (NX, NY, NZ), jnp.float32) ** steps_of(seeds[1], (NX, NY, NZ), ((0, 4), (1, 2), (2, 4)), -0.2, 0.2)), 0.5, 2.0)
    shift_field = jnp.clip(jnp.exp(math.log(2.0) - 2.0794415 * jax.random.uniform(seeds[2], (NX, NY, NZ), jnp.float32) ** steps_of(seeds[2], (NX, NY, NZ), ((0, 4), (1, 2), (2, 4)), -0.2, 0.2)), 0.25, 2.0)
    mass_field = jnp.clip(jnp.exp(math.log(2.0) - 1.3862944 * jax.random.uniform(seeds[3], (NX, NY, NZ), jnp.float32) ** steps_of(seeds[3], (NX, NY, NZ), ((0, 4), (1, 2), (2, 4)), -0.2, 0.2)), 0.5, 2.0)
    return {"start_block": start_block, "stiff_field": stiff_field, "shift_field": shift_field, "mass_field": mass_field}


def lower_solve(lower_mat, rhs):
    return lax.linalg.triangular_solve(lower_mat, rhs, left_side=True, lower=True)

def lower_trans_solve(lower_mat, rhs):
    return lax.linalg.triangular_solve(lower_mat, rhs, left_side=True, lower=True, transpose_a=True)

def hidot(left, right):
    return jnp.dot(left.astype(jnp.float32), right.astype(jnp.float32), precision=lax.Precision.HIGHEST, preferred_element_type=jnp.float32)

def gram_of(left, right):
    return hidot(left.reshape(left.shape[0], -1), right.reshape(right.shape[0], -1).T)

def combine(coeffs, vectors):
    flat = hidot(coeffs.T, vectors.reshape(vectors.shape[0], -1))
    return flat.reshape((coeffs.shape[1],) + vectors.shape[1:])

def stiffness(field, stiff_field, shift_field):
    scaled = stiff_field * field
    padded = jnp.pad(scaled, ((0, 0), (0, 0), (1, 1), (1, 1), (1, 1)))
    beside_all = padded[:, :, 2:, 1:-1, 1:-1] + padded[:, :, :-2, 1:-1, 1:-1]
    beside_all = beside_all + padded[:, :, 1:-1, 2:, 1:-1] + padded[:, :, 1:-1, :-2, 1:-1]
    beside_all = beside_all + padded[:, :, 1:-1, 1:-1, 2:] + padded[:, :, 1:-1, 1:-1, :-2]
    laplace = 6.0 * scaled - beside_all
    summed = jnp.sum(field, axis=1, keepdims=True)
    return stiff_field * laplace + shift_field * (field + 0.5 * summed)

def ritz_filter(pencil_k, pencil_m, mode_count):
    factor = jnp.linalg.cholesky(pencil_m)
    partial_value = lower_solve(factor, pencil_k)
    reduced = lower_solve(factor, partial_value.T).T
    gershgorin = jnp.max(jnp.sum(jnp.abs(reduced), axis=1))
    search = factor.T[:, :mode_count]
    for sweep_index in range(FILTER):
        search = search - hidot(reduced, search) / gershgorin
    correlation = hidot(search.T, search)
    small_factor = jnp.linalg.cholesky(correlation)
    orthonormal = lower_solve(small_factor, search.T).T
    coeffs = lower_trans_solve(factor, orthonormal)
    ritz_matrix = hidot(orthonormal.T, hidot(reduced, orthonormal))
    return (coeffs, ritz_matrix)

def reference(start_block, stiff_field, shift_field, mass_field):
    count = MODES
    start_image = stiffness(start_block, stiff_field, shift_field)
    mass_gram = gram_of(start_block, mass_field * start_block) / DOFS
    stiff_gram = gram_of(start_block, start_image) / DOFS
    factor = jnp.linalg.cholesky(mass_gram)
    current = lower_solve(factor, start_block.reshape(count, -1)).reshape(start_block.shape)
    stiff_image = lower_solve(factor, start_image.reshape(count, -1)).reshape(start_block.shape)
    ritz_matrix = lower_solve(factor, lower_solve(factor, stiff_gram).T).T
    diagonal = 6.0 * stiff_field * stiff_field + 1.5 * shift_field
    previous = None
    for iteration in range(ITERS):
        residual = (stiff_image - mass_field * combine(ritz_matrix, current)) / diagonal
        stiff_resid = stiffness(residual, stiff_field, shift_field)
        if iteration == 0:
            search_set = jnp.concatenate([current, residual], axis=0)
            image_set = jnp.concatenate([stiff_image, stiff_resid], axis=0)
        else:
            search_set = jnp.concatenate([current, residual, previous[0]], axis=0)
            image_set = jnp.concatenate([stiff_image, stiff_resid, previous[1]], axis=0)
        pencil_k = gram_of(search_set, image_set) / DOFS
        pencil_m = gram_of(search_set, mass_field * search_set) / DOFS
        coeffs, ritz_matrix = ritz_filter(pencil_k, pencil_m, count)
        current = combine(coeffs, search_set)
        stiff_image = combine(coeffs, image_set)
        previous = (combine(coeffs[count:], search_set[count:]), combine(coeffs[count:], image_set[count:]))
    return (current, ritz_matrix)
```

```python
import functools

import jax
import jax.numpy as jnp
from jax import lax
from jax.experimental import pallas as pl
from jax.experimental.pallas import tpu as pltpu
from jax.sharding import PartitionSpec as P

FILTER = 4
AXES = ("gx", "gy", "gz")
F32 = jnp.float32
BF16 = jnp.bfloat16
G_ROW, E_ROW, RHO_ROW, W_ROW, ID_ROW, GD_ROW = range(6)


def dg(a, b, ca, cb):
    return lax.dot_general(a, b, (((ca,), (cb,)), ((), ())),
                           precision=lax.Precision.HIGHEST, preferred_element_type=F32)


def nn(a, b):
    return dg(a, b, 1, 0)


def nt(a, b):
    return dg(a, b, 1, 1)


def lane_eye(rows, lanes, shift):
    return (lax.broadcasted_iota(jnp.int32, (rows, lanes), 1)
            == lax.broadcasted_iota(jnp.int32, (rows, lanes), 0) + shift).astype(F32)


def chol_inverse(mat):
    n = mat.shape[0]
    panels = n // 8
    width = 2 * n
    rows = [jnp.concatenate([mat[8 * p:8 * p + 8, :], lane_eye(8, n, 8 * p)], axis=1) for p in range(panels)]
    sub = lax.broadcasted_iota(jnp.int32, (8, width), 0)
    out = []
    for p in range(panels):
        w = rows[p]
        spread = lambda v, k: jnp.broadcast_to(v[:, 8 * p + k:8 * p + k + 1], (8, width))
        d = [spread(w, k) for k in range(8)]
        rest = {q: [spread(rows[q], k) for k in range(8)] for q in range(p + 1, panels)}
        done = jnp.zeros((8, width), F32)
        for k in range(8):
            row_of = lambda v: jnp.broadcast_to(v[k:k + 1, :], (8, width))
            pivot = row_of(d[k])
            inv = 1.0 / pivot
            at_k = sub == k
            w_row = row_of(w)
            done = jnp.where(at_k, w_row * lax.rsqrt(pivot), done)
            scaled = w_row * inv
            factor = d[k]
            w = jnp.where(at_k, scaled, w - factor * scaled)
            for j in range(k + 1, 8):
                d_row = row_of(d[j]) * inv
                d[j] = jnp.where(at_k, d_row, d[j] - factor * d_row)
        out.append(done)
        for q in range(p + 1, panels):
            for k in range(8):
                rows[q] = rows[q] - rest[q][k] * jnp.broadcast_to(w[k:k + 1, :], (8, width))
    return jnp.concatenate(out, axis=0)[:, n:]


def filtered(theta, h21, h22):
    n, m = theta.shape[0], h22.shape[0]
    h12 = h21.T
    whole = jnp.concatenate([jnp.concatenate([h22, h21], axis=1), jnp.concatenate([h12, theta], axis=1)], axis=0)
    inv = 1.0 / jnp.max(jnp.sum(jnp.abs(whole), axis=1, keepdims=True))
    search = lane_eye(n, m + n, m) - whole[m:, :] * inv
    for _ in range(FILTER - 1):
        search = search - nn(search, whole) * inv
    q = nn(chol_inverse(nt(search, search)), search)
    return q[:, m:], q[:, :m], nt(nn(q, whole), q)


def dense0_kernel(scale, gram_ref, coef_ref, theta_ref):
    v = gram_ref.shape[0]
    sbs = gram_ref[:, :v] * scale
    sks = gram_ref[:, v:] * scale
    li = chol_inverse(sbs)
    theta = nt(nn(li, sks), li)
    coef_ref[:, :v] = li
    coef_ref[:, v:] = -nn(theta, li)
    theta_ref[...] = theta


def dense1_kernel(scale, gram_ref, coef_ref, theta_ref, coef1_ref, theta1_ref):
    v = gram_ref.shape[0]
    li = coef_ref[:, :v]
    theta = theta_ref[...]
    rbs, rks, rbr, rkr = [gram_ref[:, i * v:(i + 1) * v] * scale for i in (0, 2, 1, 3)]
    lrx = nt(rbs, li)
    arx = nt(rks, li)
    jr = chol_inverse(rbr - nt(lrx, lrx))
    t = arx - nn(lrx, theta)
    f = rkr - nt(lrx, arx) - nt(t, lrx)
    h21 = nn(jr, t)
    h22 = nt(nn(jr, f), jr)
    qz, qy, ritz = filtered(theta, h21, h22)
    b = nn(qy, jr)
    a = nn(qz - nn(b, lrx), li)
    coef1_ref[:, :v] = a
    coef1_ref[:, v:2 * v] = b
    coef1_ref[:, 2 * v:3 * v] = -nn(ritz, a)
    coef1_ref[:, 3 * v:] = -nn(ritz, b)
    theta1_ref[...] = ritz


def previous_kernel(scale, gram_ref, coef1_ref, out_ref):
    v = gram_ref.shape[0]
    ab = coef1_ref[:, :2 * v]
    b = coef1_ref[:, v:2 * v]
    for i in range(2):
        part = nn(b, gram_ref[:, 2 * i * v:2 * (i + 1) * v] * scale)
        out_ref[:, 2 * i * v:(2 * i + 1) * v] = nt(part, ab)
        out_ref[:, (2 * i + 1) * v:2 * (i + 1) * v] = nt(part[:, v:], b)


def dense2_kernel(scale, gram_ref, prev_ref, coef1_ref, theta1_ref, coef2_ref, theta2_ref):
    v = gram_ref.shape[0]
    both = coef1_ref[:, :2 * v]
    a = coef1_ref[:, :v]
    b = coef1_ref[:, v:2 * v]
    theta = theta1_ref[...]
    lpx, mpp, apx, app = [prev_ref[:, i * v:(i + 1) * v] for i in range(4)]
    lrx = nt(gram_ref[:, :2 * v] * scale, both)
    arx = nt(gram_ref[:, 2 * v:4 * v] * scale, both)
    mrp = nt(gram_ref[:, v:2 * v] * scale, b)
    arp = nt(gram_ref[:, 3 * v:4 * v] * scale, b)
    rbr = gram_ref[:, 4 * v:5 * v] * scale
    rkr = gram_ref[:, 5 * v:] * scale
    jr = chol_inverse(rbr - nt(lrx, lrx))
    low = nt(mrp.T - nt(lpx, lrx), jr)
    jp = chol_inverse(mpp - nt(lpx, lpx) - nt(low, low))
    jpr = -nn(jp, nn(low, jr))
    jb = jnp.concatenate([jnp.concatenate([jr, jnp.zeros((v, v), F32)], axis=1),
                          jnp.concatenate([jpr, jp], axis=1)], axis=0)
    lx = jnp.concatenate([lrx, lpx], axis=0)
    ax = jnp.concatenate([arx, apx], axis=0)
    ab = jnp.concatenate([jnp.concatenate([rkr, arp], axis=1),
                          jnp.concatenate([arp.T, app], axis=1)], axis=0)
    t = ax - nn(lx, theta)
    f = ab - nt(lx, ax) - nt(t, lx)
    h21 = nn(jb, t)
    h22 = nt(nn(jb, f), jb)
    qz, qy, ritz = filtered(theta, h21, h22)
    cb = nn(qy, jb)
    cx = qz - nn(cb, lx)
    coef2_ref[:, :v] = nn(cx, a)
    coef2_ref[:, v:2 * v] = nn(cx + cb[:, v:], b)
    coef2_ref[:, 2 * v:3 * v] = cb[:, :v]
    coef2_ref[:, 3 * v:] = jnp.zeros((v, v), F32)
    theta2_ref[...] = ritz


def split(value):
    high = value.astype(BF16)
    return high, (value - high.astype(F32)).astype(BF16)


def bdot(a, b, cb):
    return lax.dot_general(a, b, (((1,), (cb,)), ((), ())), preferred_element_type=F32)


def mix(coef_high, coef_both, blocks):
    v = coef_high.shape[0]
    pairs = [split(block) for block in blocks]
    high = jnp.concatenate([p[0] for p in pairs], axis=0)
    low = jnp.concatenate([p[1] for p in pairs], axis=0)
    main = bdot(coef_both, high, 0)
    return main[:v] + main[v:] + bdot(coef_high, low, 0)


class Grid:
    def __init__(self, shape):
        self.v, self.c, self.nx, self.ny, self.nz = shape
        self.blocks = self.c * self.nx * self.ny
        self.lanes = self.blocks * self.nz
        self.xface = self.c * self.ny * self.nz
        self.yface = self.c * self.nx * self.nz
        assert self.blocks < self.nz and self.nz % 128 == 0 and self.ny % 2 == 0
        assert self.nx * self.nz >= 1 and self.v % 16 == 0 and max(self.ny, self.nx) <= self.v

    def block(self, c, x, y):
        return (c * self.nx + x) * self.ny + y

    def at(self, j):
        return slice(j * self.nz, (j + 1) * self.nz)


def put_faces(gd, value, c, x, y, refs, edge):
    xlo, xhi, ylo, yhi = refs
    if x == 0:
        xlo[:gd.v, gd.at(c * gd.ny + y)] = value
    if x == gd.nx - 1:
        xhi[:gd.v, gd.at(c * gd.ny + y)] = value
    if y == 0:
        ylo[:gd.v, gd.at(c * gd.nx + x)] = value
    if y == gd.ny - 1:
        yhi[:gd.v, gd.at(c * gd.nx + x)] = value
    j = gd.block(c, x, y)
    lane = lax.broadcasted_iota(jnp.int32, value.shape, 1)
    low, high = edge
    rolled_low = value if j == 0 else pltpu.roll(value, j, 1)
    rolled_high = pltpu.roll(value, (j + 1) % gd.nz, 1)
    return (jnp.where(lane == j, rolled_low, low), jnp.where(lane == j, rolled_high, high))


def stencil(gd, get, halo, coef_ref, x, y):
    xb, xa, yb, ya, zb, za = halo
    row = lambda r, xx, yy: coef_ref[r:r + 1, gd.at(xx * gd.ny + yy)]
    scaled = lambda c, xx, yy: get(c, xx, yy) * row(G_ROW, xx, yy)
    g, e = row(G_ROW, x, y), row(E_ROW, x, y)
    values = [get(c, x, y) for c in range(gd.c)]
    half = 0.5 * functools.reduce(jnp.add, values)
    lane = lax.broadcasted_iota(jnp.int32, (gd.v, gd.nz), 1)
    out = []
    for c in range(gd.c):
        j = gd.block(c, x, y)
        h = values[c] * g
        face_x, face_y = gd.at(c * gd.ny + y), gd.at(c * gd.nx + x)
        near = scaled(c, x - 1, y) if x > 0 else xb[:gd.v, face_x]
        near = near + (scaled(c, x + 1, y) if x < gd.nx - 1 else xa[:gd.v, face_x])
        near = near + (scaled(c, x, y - 1) if y > 0 else yb[:gd.v, face_y])
        near = near + (scaled(c, x, y + 1) if y < gd.ny - 1 else ya[:gd.v, face_y])
        below = jnp.broadcast_to(zb[:gd.v, j:j + 1], h.shape)
        above = jnp.broadcast_to(za[:gd.v, j:j + 1], h.shape)
        near = near + jnp.where(lane == 0, below, pltpu.roll(h, 1, 1))
        near = near + jnp.where(lane == gd.nz - 1, above, pltpu.roll(h, gd.nz - 1, 1))
        out.append(g * (6.0 * h - near) + e * (values[c] + half))
    return out


def gram_of(left_both, right_high, right_low):
    v = left_both.shape[0] // 2
    main = bdot(left_both[...], right_high[...], 1)
    return main[:v] + main[v:] + bdot(left_both[:v, :], right_low[...], 1)


def pack_kernel(gd, s_ref, g_ref, e_ref, rho_ref, sm_ref, coef_ref, xlo, xhi, ylo, yhi, zlo, zhi):
    v, nz = gd.v, gd.nz
    coef_ref[...] = jnp.zeros(coef_ref.shape, F32)
    for ref, used in ((xlo, gd.xface), (xhi, gd.xface), (ylo, gd.yface), (yhi, gd.yface)):
        ref[:, used:] = jnp.zeros((v, nz), F32)
    w_lane = lax.broadcasted_iota(jnp.int32, (8, nz), 1)
    w_low = jnp.zeros((8, nz), F32)
    w_high = jnp.zeros((8, nz), F32)
    for x in range(gd.nx):
        for y in range(gd.ny):
            r = x * gd.ny + y
            g, e, rho = (ref[r:r + 1, :] for ref in (g_ref, e_ref, rho_ref))
            inverse = 1.0 / (6.0 * g * g + 1.5 * e)
            w = rho * inverse
            for i, value in enumerate((g, e, rho, w, inverse, g * inverse)):
                coef_ref[i:i + 1, gd.at(r)] = value
            if x == 0:
                xlo[y:y + 1, gd.xface:] = w
            if x == gd.nx - 1:
                xhi[y:y + 1, gd.xface:] = w
            if y == 0:
                ylo[x:x + 1, gd.yface:] = w
            if y == gd.ny - 1:
                yhi[x:x + 1, gd.yface:] = w
            wide = jnp.broadcast_to(w, (8, nz))
            for c in range(gd.c):
                j = gd.block(c, x, y)
                w_low = jnp.where(w_lane == j, pltpu.roll(wide, j, 1) if j else wide, w_low)
                w_high = jnp.where(w_lane == j, pltpu.roll(wide, (j + 1) % nz, 1), w_high)
    edge = (jnp.zeros((v, nz), F32), jnp.zeros((v, nz), F32))
    for c in range(gd.c):
        for x in range(gd.nx):
            for y in range(gd.ny):
                j = gd.block(c, x, y)
                value = s_ref[pl.ds(j, v, stride=gd.blocks), :]
                sm_ref[:, gd.at(j)] = value
                edge = put_faces(gd, value * coef_ref[G_ROW:G_ROW + 1, gd.at(x * gd.ny + y)], c, x, y,
                                 (xlo, xhi, ylo, yhi), edge)
    zlo[:v, :], zhi[:v, :] = edge
    zlo[v:, :] = w_low
    zhi[v:, :] = w_high


def image_kernel(gd, sm_ref, coef_ref, xb, xa, yb, ya, zb, za,
                 ks_ref, gram_ref, xlo, xhi, ylo, yhi, zlo, zhi, left, right_high, right_low):
    v = gd.v
    get = lambda c, x, y: sm_ref[:, gd.at(gd.block(c, x, y))]
    edge = (jnp.zeros((v, gd.nz), F32), jnp.zeros((v, gd.nz), F32))
    for x in range(gd.nx):
        for y in range(gd.ny):
            r = gd.at(x * gd.ny + y)
            images = stencil(gd, get, (xb, xa, yb, ya, zb, za), coef_ref, x, y)
            for c in range(gd.c):
                at = gd.at(gd.block(c, x, y))
                value = get(c, x, y)
                ks_ref[:, at] = images[c]
                edge = put_faces(gd, images[c] * coef_ref[GD_ROW:GD_ROW + 1, r], c, x, y, (xlo, xhi, ylo, yhi), edge)
                left[:v, at], left[v:, at] = split(value)
                for i, part in enumerate((value * coef_ref[RHO_ROW:RHO_ROW + 1, r], images[c])):
                    right_high[i * v:(i + 1) * v, at], right_low[i * v:(i + 1) * v, at] = split(part)
    zlo[...], zhi[...] = edge
    gram_ref[...] = gram_of(left, right_high, right_low)


def coefficients(coef_ref, both_ref):
    v = coef_ref.shape[0]
    both_ref[:v, :], both_ref[v:, :] = split(coef_ref[...])


def residual_kernel(gd, last, depth, *refs):
    v, nz = gd.v, gd.nz
    refs = list(refs)
    take = lambda n: [refs.pop(0) for _ in range(n)]
    (mix_ref, coef_ref) = take(2)
    images, vectors = take(depth), take(depth)
    image_halo = [take(6) for _ in range(depth)]
    vector_halo = [take(6) for _ in range(depth)]
    if last:
        r_ref, gram_ref = take(2)
        halo = take(6)
    else:
        r_ref, kr_ref, gram_ref = take(3)
        halo = take(6)
        faces = take(6)
    both, left, right_high, right_low = take(4)
    both[:v, :], both[v:, :] = split(mix_ref[...])
    mixed = lambda a, b: mix(both[:v, :], both[...], a + b)
    first = vector_halo[0]

    def interior(c, _):
        for i in range(gd.nx * gd.ny // 2):
            at = pl.ds(pl.multiple_of(c * gd.nx * gd.ny * nz + 2 * i * nz, 2 * nz), 2 * nz)
            row = slice(2 * i * nz, 2 * (i + 1) * nz)
            inverse, w = coef_ref[ID_ROW:ID_ROW + 1, row], coef_ref[W_ROW:W_ROW + 1, row]
            r_ref[:, at] = mixed([ref[:, at] * inverse for ref in images], [ref[:, at] * w for ref in vectors])
        return 0

    def xfaces(c, _):
        for side in range(2):
            for i in range(gd.ny // 2):
                at = pl.ds(pl.multiple_of(c * gd.ny * nz + 2 * i * nz, 2 * nz), 2 * nz)
                w = jnp.concatenate([first[side][k:k + 1, gd.xface:] for k in (2 * i, 2 * i + 1)], axis=1)
                halo[side][:, at] = mixed([h[side][:v, at] for h in image_halo],
                                          [h[side][:v, at] * w for h in vector_halo])
        return 0

    lax.fori_loop(0, gd.c, xfaces, 0)
    for side in (2, 3):
        for j in range(gd.c * gd.nx):
            at = gd.at(j)
            w = first[side][j % gd.nx:j % gd.nx + 1, gd.yface:]
            halo[side][:, at] = mixed([h[side][:v, at] for h in image_halo], [h[side][:v, at] * w for h in vector_halo])
    for side in (4, 5):
        w = first[side][v:v + 1, :]
        halo[side][...] = mixed([h[side][:v, :] for h in image_halo], [h[side][:v, :] * w for h in vector_halo])
    lax.fori_loop(0, gd.c, interior, 0)

    get = lambda c, x, y: r_ref[:, gd.at(gd.block(c, x, y))]
    edge = (jnp.zeros((v, nz), F32), jnp.zeros((v, nz), F32))
    for x in range(gd.nx):
        for y in range(gd.ny):
            r = gd.at(x * gd.ny + y)
            rho = coef_ref[RHO_ROW:RHO_ROW + 1, r]
            stiff = stencil(gd, get, halo, coef_ref, x, y)
            for c in range(gd.c):
                at = gd.at(gd.block(c, x, y))
                value = get(c, x, y)
                if not last:
                    kr_ref[:, at] = stiff[c]
                    edge = put_faces(gd, stiff[c] * coef_ref[GD_ROW:GD_ROW + 1, r], c, x, y, faces[:4], edge)
                left[:v, at], left[v:, at] = split(value)
                parts = [ref[:, at] * rho for ref in vectors] + [ref[:, at] for ref in images]
                place = depth if not last else 2 * depth
                parts.insert(place, value * rho)
                parts.append(stiff[c])
                for i, part in enumerate(parts):
                    right_high[i * v:(i + 1) * v, at], right_low[i * v:(i + 1) * v, at] = split(part)
    if not last:
        faces[4][...], faces[5][...] = edge
    gram_ref[...] = gram_of(left, right_high, right_low)


def final_kernel(gd, mix_ref, s_ref, r0_ref, r1_ref, out_ref, both):
    v, nz = gd.v, gd.nz
    k = 3 * v
    both[:v, :], both[v:, :] = split(mix_ref[...])
    high, pair = both[:v, :k], both[:, :k]
    for j in range(0, gd.blocks, 2):
        at = slice(j * nz, (j + 2) * nz)
        value = mix(high, pair, [s_ref[:, at], r0_ref[:, at], r1_ref[:, at]])
        out_ref[pl.ds(j, v, stride=gd.blocks), :] = value[:, :nz]
        out_ref[pl.ds(j + 1, v, stride=gd.blocks), :] = value[:, nz:]


def call(kernel, outs, args, scratch=(), flops=1 << 20, vmem=40 << 20):
    spec = pl.BlockSpec(memory_space=pltpu.VMEM)
    results = pl.pallas_call(
        kernel,
        out_shape=[jax.ShapeDtypeStruct(s, F32) for s in outs],
        in_specs=[spec] * len(args),
        out_specs=[spec] * len(outs),
        scratch_shapes=[pltpu.VMEM(s, d) for s, d in scratch],
        compiler_params=pltpu.CompilerParams(vmem_limit_bytes=vmem),
        cost_estimate=pl.CostEstimate(flops=flops, bytes_accessed=1 << 20, transcendentals=0),
    )(*args)
    return list(results)


def exchange(faces):
    out = []
    for axis, (low, high) in zip(AXES, zip(faces[::2], faces[1::2])):
        n = lax.axis_size(axis)
        up = [(i, i + 1) for i in range(n - 1)]
        down = [(j, i) for i, j in up]
        out.append(lax.ppermute(high, axis, up))
        out.append(lax.ppermute(low, axis, down))
    return out


def sum_over(x, axis):
    n = lax.axis_size(axis)
    if n & (n - 1):
        return lax.psum(x, axis)
    if n <= 4:
        parts = [lax.ppermute(x, axis, [(i, i ^ s) for i in range(n)]) for s in range(1, n)]
        return functools.reduce(jnp.add, parts, x)
    step = 1
    while step < n:
        x = x + lax.ppermute(x, axis, [(i, i ^ step) for i in range(n)])
        step *= 2
    return x


def total(x):
    n = lax.axis_size("gy")
    if n != 2:
        return sum_over(sum_over(sum_over(x, "gy"), "gx"), "gz")
    half = x.shape[0] // 2
    me = lax.axis_index("gy")
    swap = [(0, 1), (1, 0)]
    piece = lambda k: lax.dynamic_slice_in_dim(x, k * half, half, 0)
    mine = piece(me) + lax.ppermute(piece(1 - me), "gy", swap)
    mine = sum_over(sum_over(mine, "gx"), "gz")
    theirs = lax.ppermute(mine, "gy", swap)
    return jnp.where(me == 0, jnp.concatenate([mine, theirs], 0), jnp.concatenate([theirs, mine], 0))


def local(start_block, stiff_field, shift_field, mass_field):
    gd = Grid(start_block.shape)
    v, nz, lanes = gd.v, gd.nz, gd.lanes
    nodes = stiff_field.size
    count = nodes * gd.c
    for axis in AXES:
        count *= lax.axis_size(axis)
    scale = 1.0 / count
    rows = gd.nx * gd.ny
    fields = [f.reshape(rows, nz) for f in (stiff_field, shift_field, mass_field)]
    first_faces = [(v, gd.xface + nz)] * 2 + [(v, gd.yface + nz)] * 2 + [(v + 8, nz)] * 2
    faces = [(v, gd.xface)] * 2 + [(v, gd.yface)] * 2 + [(v, nz)] * 2
    full = (v, lanes)

    packed = call(functools.partial(pack_kernel, gd), [full, (8, rows * nz)] + first_faces,
                  [start_block.reshape(v * gd.blocks, nz)] + fields)
    sm, coef = packed[:2]
    halo_s = exchange(packed[2:])
    gram_scratch = lambda n: [((2 * v, lanes), BF16), ((n * v, lanes), BF16), ((n * v, lanes), BF16)]
    imaged = call(functools.partial(image_kernel, gd), [full, (v, 2 * v)] + faces,
                  [sm, coef] + halo_s, gram_scratch(2), flops=1 << 28)
    ks, gram0 = imaged[:2]
    halo_u = exchange(imaged[2:])
    coef0, theta0 = call(functools.partial(dense0_kernel, scale), [(v, 2 * v), (v, v)], [total(gram0)])

    res = call(functools.partial(residual_kernel, gd, False, 1),
               [full, full, (v, 4 * v)] + faces + faces,
               [coef0, coef, ks, sm] + halo_u + halo_s,
               [((2 * v, 2 * v), BF16)] + gram_scratch(4), flops=1 << 29)
    r0, kr0, gram1 = res[:3]
    halo_r, halo_b = res[3:9], exchange(res[9:])
    gram1 = total(gram1)
    coef1, theta1 = call(functools.partial(dense1_kernel, scale), [(v, 4 * v), (v, v)], [gram1, coef0, theta0])

    res = call(functools.partial(residual_kernel, gd, True, 2),
               [full, (v, 6 * v)] + faces,
               [coef1, coef, ks, kr0, sm, r0] + halo_u + halo_b + halo_s + halo_r,
               [((2 * v, 4 * v), BF16)] + gram_scratch(6), flops=1 << 29, vmem=56 << 20)
    r1, gram2 = res[:2]
    (prev,) = call(functools.partial(previous_kernel, scale), [(v, 4 * v)], [gram1, coef1])
    coef2, theta2 = call(functools.partial(dense2_kernel, scale), [(v, 4 * v), (v, v)],
                         [total(gram2), prev, coef1, theta1])
    (modes,) = call(functools.partial(final_kernel, gd), [(v * gd.blocks, nz)],
                    [coef2, sm, r0, r1], [((2 * v, 4 * v), BF16)])
    return modes.reshape(start_block.shape), theta2


def solution(mesh):
    grid = P("gx", "gy", "gz")
    block = P(None, None, "gx", "gy", "gz")
    return jax.shard_map(local, mesh=mesh, in_specs=(block, grid, grid, grid),
                         out_specs=(block, P()), check_vma=False)
```

```python
import functools

import jax
import jax.numpy as jnp
from jax import lax
from jax.experimental import pallas as pl
from jax.experimental.pallas import tpu as pltpu
from jax.sharding import PartitionSpec as P


FILTER = 4
AXES = ("gx", "gy", "gz")
F32 = jnp.float32
BF16 = jnp.bfloat16
G_ROW, E_ROW, RHO_ROW, W_ROW, ID_ROW, GD_ROW = range(6)


def dg(a, b, ca, cb):
    return lax.dot_general(a, b, (((ca,), (cb,)), ((), ())),
                           precision=lax.Precision.HIGHEST, preferred_element_type=F32)


def nn(a, b):
    return dg(a, b, 1, 0)


def nt(a, b):
    return dg(a, b, 1, 1)


def lane_eye(rows, lanes, shift):
    return (lax.broadcasted_iota(jnp.int32, (rows, lanes), 1)
            == lax.broadcasted_iota(jnp.int32, (rows, lanes), 0) + shift).astype(F32)


def chol_inverse(mat):
    n = mat.shape[0]
    panels = n // 8
    width = 2 * n
    rows = [jnp.concatenate([mat[8 * p:8 * p + 8, :], lane_eye(8, n, 8 * p)], axis=1) for p in range(panels)]
    sub = lax.broadcasted_iota(jnp.int32, (8, width), 0)
    out = []
    for p in range(panels):
        w = rows[p]
        spread = lambda v, k: jnp.broadcast_to(v[:, 8 * p + k:8 * p + k + 1], (8, width))
        d = [spread(w, k) for k in range(8)]
        rest = {q: [spread(rows[q], k) for k in range(8)] for q in range(p + 1, panels)}
        done = jnp.zeros((8, width), F32)
        for k in range(8):
            row_of = lambda v: jnp.broadcast_to(v[k:k + 1, :], (8, width))
            pivot = row_of(d[k])
            inv = 1.0 / pivot
            at_k = sub == k
            w_row = row_of(w)
            done = jnp.where(at_k, w_row * lax.rsqrt(pivot), done)
            scaled = w_row * inv
            factor = d[k]
            w = jnp.where(at_k, scaled, w - factor * scaled)
            for j in range(k + 1, 8):
                d_row = row_of(d[j]) * inv
                d[j] = jnp.where(at_k, d_row, d[j] - factor * d_row)
        out.append(done)
        for q in range(p + 1, panels):
            for k in range(8):
                rows[q] = rows[q] - rest[q][k] * jnp.broadcast_to(w[k:k + 1, :], (8, width))
    return jnp.concatenate(out, axis=0)[:, n:]


def filtered(theta, h21, h22):
    n, m = theta.shape[0], h22.shape[0]
    h12 = h21.T
    whole = jnp.concatenate([jnp.concatenate([h22, h21], axis=1), jnp.concatenate([h12, theta], axis=1)], axis=0)
    inv = 1.0 / jnp.max(jnp.sum(jnp.abs(whole), axis=1, keepdims=True))
    search = lane_eye(n, m + n, m) - whole[m:, :] * inv
    for _ in range(FILTER - 1):
        search = search - nn(search, whole) * inv
    q = nn(chol_inverse(nt(search, search)), search)
    return q[:, m:], q[:, :m], nt(nn(q, whole), q)


def dense0_kernel(scale, gram_ref, coef_ref, theta_ref):
    v = gram_ref.shape[0]
    sbs = gram_ref[:, :v] * scale
    sks = gram_ref[:, v:] * scale
    li = chol_inverse(sbs)
    theta = nt(nn(li, sks), li)
    coef_ref[:, :v] = li
    coef_ref[:, v:] = -nn(theta, li)
    theta_ref[...] = theta


def dense1_kernel(scale, gram_ref, coef_ref, theta_ref, coef1_ref, theta1_ref):
    v = gram_ref.shape[0]
    li = coef_ref[:, :v]
    theta = theta_ref[...]
    rbs, rks, rbr, rkr = [gram_ref[:, i * v:(i + 1) * v] * scale for i in (0, 2, 1, 3)]
    lrx = nt(rbs, li)
    arx = nt(rks, li)
    jr = chol_inverse(rbr - nt(lrx, lrx))
    t = arx - nn(lrx, theta)
    f = rkr - nt(lrx, arx) - nt(t, lrx)
    h21 = nn(jr, t)
    h22 = nt(nn(jr, f), jr)
    qz, qy, ritz = filtered(theta, h21, h22)
    b = nn(qy, jr)
    a = nn(qz - nn(b, lrx), li)
    coef1_ref[:, :v] = a
    coef1_ref[:, v:2 * v] = b
    coef1_ref[:, 2 * v:3 * v] = -nn(ritz, a)
    coef1_ref[:, 3 * v:] = -nn(ritz, b)
    theta1_ref[...] = ritz


def previous_kernel(scale, gram_ref, coef1_ref, out_ref):
    v = gram_ref.shape[0]
    ab = coef1_ref[:, :2 * v]
    b = coef1_ref[:, v:2 * v]
    for i in range(2):
        part = nn(b, gram_ref[:, 2 * i * v:2 * (i + 1) * v] * scale)
        out_ref[:, 2 * i * v:(2 * i + 1) * v] = nt(part, ab)
        out_ref[:, (2 * i + 1) * v:2 * (i + 1) * v] = nt(part[:, v:], b)


def dense2_kernel(scale, gram_ref, prev_ref, coef1_ref, theta1_ref, coef2_ref, theta2_ref):
    v = gram_ref.shape[0]
    both = coef1_ref[:, :2 * v]
    a = coef1_ref[:, :v]
    b = coef1_ref[:, v:2 * v]
    theta = theta1_ref[...]
    lpx, mpp, apx, app = [prev_ref[:, i * v:(i + 1) * v] for i in range(4)]
    lrx = nt(gram_ref[:, :2 * v] * scale, both)
    arx = nt(gram_ref[:, 2 * v:4 * v] * scale, both)
    mrp = nt(gram_ref[:, v:2 * v] * scale, b)
    arp = nt(gram_ref[:, 3 * v:4 * v] * scale, b)
    rbr = gram_ref[:, 4 * v:5 * v] * scale
    rkr = gram_ref[:, 5 * v:] * scale
    jr = chol_inverse(rbr - nt(lrx, lrx))
    low = nt(mrp.T - nt(lpx, lrx), jr)
    jp = chol_inverse(mpp - nt(lpx, lpx) - nt(low, low))
    jpr = -nn(jp, nn(low, jr))
    jb = jnp.concatenate([jnp.concatenate([jr, jnp.zeros((v, v), F32)], axis=1),
                          jnp.concatenate([jpr, jp], axis=1)], axis=0)
    lx = jnp.concatenate([lrx, lpx], axis=0)
    ax = jnp.concatenate([arx, apx], axis=0)
    ab = jnp.concatenate([jnp.concatenate([rkr, arp], axis=1),
                          jnp.concatenate([arp.T, app], axis=1)], axis=0)
    t = ax - nn(lx, theta)
    f = ab - nt(lx, ax) - nt(t, lx)
    h21 = nn(jb, t)
    h22 = nt(nn(jb, f), jb)
    qz, qy, ritz = filtered(theta, h21, h22)
    cb = nn(qy, jb)
    cx = qz - nn(cb, lx)
    coef2_ref[:, :v] = nn(cx, a)
    coef2_ref[:, v:2 * v] = nn(cx + cb[:, v:], b)
    coef2_ref[:, 2 * v:3 * v] = cb[:, :v]
    coef2_ref[:, 3 * v:] = jnp.zeros((v, v), F32)
    theta2_ref[...] = ritz


def split(value):
    high = value.astype(BF16)
    return high, (value - high.astype(F32)).astype(BF16)


def bdot(a, b, cb):
    return lax.dot_general(a, b, (((1,), (cb,)), ((), ())), preferred_element_type=F32)


def mix(coef_high, coef_both, blocks):
    v = coef_high.shape[0]
    pairs = [split(block) for block in blocks]
    high = jnp.concatenate([p[0] for p in pairs], axis=0)
    low = jnp.concatenate([p[1] for p in pairs], axis=0)
    main = bdot(coef_both, high, 0)
    return main[:v] + main[v:] + bdot(coef_high, low, 0)


class Grid:
    def __init__(self, shape, n, ycount):
        self.ysides = 1 if ycount == 2 else 2
        self.v, self.c, self.nx, self.ny, self.nz = shape
        self.n = n
        self.part = self.nz // n
        self.blocks = self.c * self.nx * self.ny
        self.lanes = self.blocks * self.nz
        self.yface = self.c * self.nx * self.nz
        self.zface = self.nz * (-(-self.blocks // self.part))
        self.message = self.lanes // n
        assert self.nz % 128 == 0 and self.nz % n == 0 and n & (n - 1) == 0
        pieces = self.ysides * self.c * self.nx + 2 * (self.zface // self.nz)
        self.columns = max(-(-pieces // n), self.nx * self.ny // n)
        assert self.ny % n == 0 and self.ny % 2 == 0 and self.nx > 1 and self.v % 16 == 0 and self.nx <= 8

    def block(self, c, x, y):
        return (c * self.nx + x) * self.ny + y

    def at(self, j):
        return slice(j * self.nz, (j + 1) * self.nz)

    def group_of(self, rows):
        return lax.broadcasted_iota(jnp.int32, (rows, self.nz), 1) // self.part

    def place_of(self, rows):
        return lax.broadcasted_iota(jnp.int32, (rows, self.nz), 1) % self.part


def turn(value, shift):
    shift %= value.shape[1]
    return pltpu.roll(value, shift, 1) if shift else value


def to_group(gd, value, source, target):
    return pltpu.roll(value, ((target - source) & (gd.n - 1)) * gd.part, 1)


def put_yfaces(gd, my, rows, get, refs):
    for c in range(gd.c):
        for x in range(gd.nx):
            at = gd.at(c * gd.nx + x)
            low, high = get(c, x, 0), get(c, x, gd.ny - 1)
            if gd.ysides == 1:
                refs[0][:rows, at] = jnp.where(my == 0, high, low)
            else:
                refs[0][:rows, at] = low
                refs[1][:rows, at] = high


class Edges:
    def __init__(self, gd, rows):
        self.gd = gd
        columns = gd.zface // gd.nz
        self.low = [jnp.zeros((rows, gd.nz), F32)] * columns
        self.high = [jnp.zeros((rows, gd.nz), F32)] * columns
        self.place = gd.place_of(rows)

    def add(self, value, j, low_turn=0, high_turn=None):
        gd = self.gd
        column, place = j // gd.part, j % gd.part
        here = self.place == place
        high_turn = 1 - gd.part if high_turn is None else high_turn
        self.low[column] = jnp.where(here, turn(value, place + low_turn), self.low[column])
        self.high[column] = jnp.where(here, turn(value, place + high_turn), self.high[column])

    def finish(self, zlo, zhi):
        for i in range(len(self.low)):
            zlo[:, self.gd.at(i)] = self.low[i]
            zhi[:, self.gd.at(i)] = self.high[i]


def stencil(gd, my, get, halo, coef_ref, x, y):
    zb, za = halo[-2:]
    if gd.ysides == 1:
        before = lambda face: jnp.where(my == 0, 0.0, halo[0][:gd.v, face])
        after = lambda face: jnp.where(my == 0, halo[0][:gd.v, face], 0.0)
    else:
        before = lambda face: halo[0][:gd.v, face]
        after = lambda face: halo[1][:gd.v, face]
    row = lambda r, xx, yy: coef_ref[r:r + 1, gd.at(xx * gd.ny + yy)]
    scaled = lambda c, xx, yy: get(c, xx, yy) * row(G_ROW, xx, yy)
    g, e = row(G_ROW, x, y), row(E_ROW, x, y)
    values = [get(c, x, y) for c in range(gd.c)]
    half = 0.5 * functools.reduce(jnp.add, values)
    group, place = gd.group_of(gd.v), gd.place_of(gd.v)
    out = []
    for c in range(gd.c):
        j = gd.block(c, x, y)
        h = values[c] * g
        face = gd.at(c * gd.nx + x)
        if x > 0:
            near = scaled(c, x - 1, y)
        else:
            near = jnp.where(group == 0, 0.0, turn(scaled(c, gd.nx - 1, y), gd.part))
        if x < gd.nx - 1:
            near = near + scaled(c, x + 1, y)
        else:
            near = near + jnp.where(group == gd.n - 1, 0.0, turn(scaled(c, 0, y), -gd.part))
        near = near + (scaled(c, x, y - 1) if y > 0 else before(face))
        near = near + (scaled(c, x, y + 1) if y < gd.ny - 1 else after(face))
        column, at = gd.at(j // gd.part), j % gd.part
        near = near + jnp.where(place == 0, turn(zb[:gd.v, column], -at), turn(h, 1))
        near = near + jnp.where(place == gd.part - 1, turn(za[:gd.v, column], gd.part - 1 - at), turn(h, -1))
        out.append(g * (6.0 * h - near) + e * (values[c] + half))
    return out


def gram_of(left_both, right_high, right_low):
    v = left_both.shape[0] // 2
    main = bdot(left_both[...], right_high[...], 1)
    return main[:v] + main[v:] + bdot(left_both[:v, :], right_low[...], 1)


def scatter(gd, me, rows, pieces, out_refs, at, out_rows=slice(None)):
    group = gd.group_of(rows)
    for s in range(gd.n):
        target = me ^ s
        value = None
        for q in range(gd.n):
            moved = to_group(gd, pieces[q], target, q)
            value = moved if q == 0 else jnp.where(group == q, moved, value)
        out_refs[s][out_rows, at] = value


def gather(gd, me, rows, values, q):
    group = gd.group_of(rows)
    block = None
    for s in range(gd.n):
        source = me ^ s
        moved = to_group(gd, values[s], q, source)
        block = moved if s == 0 else jnp.where(group == source, moved, block)
    return block


def lanes_of(gd, j):
    return pl.ds(pl.multiple_of(j * gd.nz, gd.nz), gd.nz)


def send_kernel(gd, me_ref, *refs):
    sources, messages = refs[:4], refs[4:4 + gd.n]
    yfaces = refs[4 + gd.n:4 + gd.n + gd.ysides]
    zlo, zhi, field_ref, s_ref, sems = refs[4 + gd.n + gd.ysides:]
    me, v, nz, rows = me_ref[0], gd.v, gd.nz, gd.nx * gd.ny
    targets = [s_ref] + [field_ref.at[f * rows:(f + 1) * rows] for f in range(3)]
    copies = [pltpu.make_async_copy(a, b, sems.at[i]) for i, (a, b) in enumerate(zip(sources, targets))]
    for copy in copies:
        copy.start()
    for copy in copies:
        copy.wait()

    def column(i, _):
        scatter(gd, me, v, [s_ref[pl.ds(i * gd.n + q, v, stride=gd.blocks), :] for q in range(gd.n)],
                messages, lanes_of(gd, i))
        return 0

    lax.fori_loop(0, gd.blocks // gd.n, column, 0, unroll=2)
    field = lambda f, r: field_ref[f * rows + r:f * rows + r + 1, :]

    def tall(c, x, y):
        r = x * gd.ny + y
        g = field(0, r)
        w = jnp.broadcast_to(field(2, r) / (6.0 * g * g + 1.5 * field(1, r)), (8, nz))
        return jnp.concatenate([s_ref[pl.ds(gd.block(c, x, y), v, stride=gd.blocks), :] * g, w], axis=0)

    put_yfaces(gd, me_ref[1], v + 8, tall, yfaces)
    edges = Edges(gd, v + 8)
    for x in range(gd.nx):
        for y in range(gd.ny):
            for c in range(gd.c):
                edges.add(tall(c, x, y), gd.block(c, x, y), 1, -gd.part)
    edges.finish(zlo, zhi)


def halo_kernel(gd, me_ref, *refs):
    yfaces = refs[:gd.ysides]
    zlo, zhi, zlo_in, zhi_in, field_ref = refs[gd.ysides:gd.ysides + 5]
    messages = refs[gd.ysides + 5:]
    me, rows, nz = me_ref[0], gd.v + 8, gd.nz
    group = gd.group_of(rows)
    pieces = [ref[:, gd.at(j)] for ref in yfaces for j in range(gd.c * gd.nx)]
    for own, other, at in ((zlo, zlo_in, 0), (zhi, zhi_in, gd.n - 1)):
        pieces += [jnp.where(group == at, other[:, gd.at(i)], own[:, gd.at(i)]) for i in range(gd.zface // nz)]
    pieces += [pieces[-1]] * (gd.columns * gd.n - len(pieces))
    for i in range(gd.columns):
        scatter(gd, me, rows, pieces[gd.n * i:gd.n * (i + 1)], messages, gd.at(i))
    for f in range(3):
        for i in range(gd.nx * gd.ny // gd.n):
            row = f * gd.nx * gd.ny + gd.n * i
            scatter(gd, me, 1, [field_ref[row + q:row + q + 1, :] for q in range(gd.n)], messages, gd.at(i),
                    slice(gd.v + 1 + f, gd.v + 2 + f))


def receive_kernel(gd, me_ref, *refs):
    messages, halo_messages = refs[:gd.n], refs[gd.n:2 * gd.n]
    sm_ref, coef_ref, *halo = refs[2 * gd.n:]
    me, v, nz = me_ref[0], gd.v, gd.nz
    for i in range(gd.nx * gd.ny // gd.n):
        values = [m[v:, gd.at(i)] for m in halo_messages]
        for q in range(gd.n):
            block = gather(gd, me, 8, values, q)
            g, e, rho = (block[k:k + 1] for k in (1, 2, 3))
            inverse = 1.0 / (6.0 * g * g + 1.5 * e)
            for k, value in enumerate((g, e, rho, rho * inverse, inverse, g * inverse)):
                coef_ref[k:k + 1, gd.at(gd.n * i + q)] = value
    targets = [(ref, j) for ref in halo[:-2] for j in range(gd.c * gd.nx)]
    targets += [(ref, i) for ref in halo[-2:] for i in range(gd.zface // nz)]
    for t, (ref, j) in enumerate(targets):
        ref[:, gd.at(j)] = gather(gd, me, v + 8, [m[:, gd.at(t // gd.n)] for m in halo_messages], t % gd.n)

    def column(i, _):
        values = [m[:, lanes_of(gd, i)] for m in messages]
        for q in range(gd.n):
            sm_ref[:, lanes_of(gd, i * gd.n + q)] = gather(gd, me, v, values, q)
        return 0

    lax.fori_loop(0, gd.blocks // gd.n, column, 0, unroll=2)


def image_kernel(gd, me_ref, sm_ref, coef_ref, *refs):
    sides = gd.ysides + 2
    halo, (ks_ref, gram_ref), faces = refs[:sides], refs[sides:sides + 2], refs[sides + 2:2 * sides + 2]
    left, right_high, right_low = refs[2 * sides + 2:]
    v = gd.v
    get = lambda c, x, y: sm_ref[:, gd.at(gd.block(c, x, y))]
    factor = lambda x, y: coef_ref[GD_ROW:GD_ROW + 1, gd.at(x * gd.ny + y)]
    edges = Edges(gd, v)
    for x in range(gd.nx):
        for y in range(gd.ny):
            rho = coef_ref[RHO_ROW:RHO_ROW + 1, gd.at(x * gd.ny + y)]
            images = stencil(gd, me_ref[1], get, halo, coef_ref, x, y)
            for c in range(gd.c):
                at = gd.at(gd.block(c, x, y))
                value = get(c, x, y)
                ks_ref[:, at] = images[c]
                edges.add(images[c] * factor(x, y), gd.block(c, x, y))
                left[:v, at], left[v:, at] = split(value)
                for i, part in enumerate((value * rho, images[c])):
                    right_high[i * v:(i + 1) * v, at], right_low[i * v:(i + 1) * v, at] = split(part)
    edges.finish(*faces[-2:])
    put_yfaces(gd, me_ref[1], v, lambda c, x, y: ks_ref[:, gd.at(gd.block(c, x, y))] * factor(x, y), faces)
    gram_ref[...] = gram_of(left, right_high, right_low)


def residual_kernel(gd, last, depth, me_ref, *refs):
    v, nz = gd.v, gd.nz
    refs = list(refs)
    take = lambda n: [refs.pop(0) for _ in range(n)]
    (mix_ref, coef_ref) = take(2)
    images, vectors = take(depth), take(depth)
    sides = gd.ysides + 2
    image_halo = [take(sides) for _ in range(depth)]
    vector_halo = [take(sides) for _ in range(depth)]
    if last:
        gram_ref, messages = take(1)[0], take(gd.n)
    else:
        r_ref, kr_ref, gram_ref = take(3)
        messages = take(gd.n)
        halo, faces = take(sides), take(sides)
        edges = Edges(gd, v)
    both, left, right_high, right_low = take(4)
    if last:
        r_ref, halo = take(1)[0], take(sides)
    both[:v, :], both[v:, :] = split(mix_ref[...])
    mixed = lambda a, b: mix(both[:v, :], both[...], a + b)
    first = vector_halo[0]

    def interior(c, _):
        for i in range(gd.nx * gd.ny // 2):
            at = pl.ds(pl.multiple_of(c * gd.nx * gd.ny * nz + 2 * i * nz, 2 * nz), 2 * nz)
            row = slice(2 * i * nz, 2 * (i + 1) * nz)
            inverse, w = coef_ref[ID_ROW:ID_ROW + 1, row], coef_ref[W_ROW:W_ROW + 1, row]
            r_ref[:, at] = mixed([ref[:, at] * inverse for ref in images], [ref[:, at] * w for ref in vectors])
        return 0

    for side in range(gd.ysides):
        for j in range(gd.c * gd.nx):
            at = gd.at(j)
            w = first[side][v:v + 1, at]
            halo[side][:, at] = mixed([h[side][:v, at] for h in image_halo], [h[side][:v, at] * w for h in vector_halo])
    for side in (gd.ysides, gd.ysides + 1):
        w = first[side][v:v + 1, :]
        halo[side][...] = mixed([h[side][:v, :] for h in image_halo], [h[side][:v, :] * w for h in vector_halo])
    lax.fori_loop(0, gd.c, interior, 0)
    me = me_ref[0]

    def column(i, _):
        scatter(gd, me, v, [r_ref[:, lanes_of(gd, i * gd.n + q)] for q in range(gd.n)], messages, lanes_of(gd, i))
        return 0

    lax.fori_loop(0, gd.blocks // gd.n, column, 0)
    get = lambda c, x, y: r_ref[:, gd.at(gd.block(c, x, y))]
    for x in range(gd.nx):
        for y in range(gd.ny):
            r = gd.at(x * gd.ny + y)
            rho = coef_ref[RHO_ROW:RHO_ROW + 1, r]
            stiff = stencil(gd, me_ref[1], get, halo, coef_ref, x, y)
            for c in range(gd.c):
                at = gd.at(gd.block(c, x, y))
                value = get(c, x, y)
                if not last:
                    kr_ref[:, at] = stiff[c]
                    edges.add(stiff[c] * coef_ref[GD_ROW:GD_ROW + 1, r], gd.block(c, x, y))
                left[:v, at], left[v:, at] = split(value)
                parts = [ref[:, at] * rho for ref in vectors] + [ref[:, at] for ref in images]
                place = depth if not last else 2 * depth
                parts.insert(place, value * rho)
                parts.append(stiff[c])
                for i, part in enumerate(parts):
                    right_high[i * v:(i + 1) * v, at], right_low[i * v:(i + 1) * v, at] = split(part)
    if not last:
        edges.finish(*faces[-2:])
        put_yfaces(gd, me_ref[1], v, lambda c, x, y: kr_ref[:, gd.at(gd.block(c, x, y))]
                   * coef_ref[GD_ROW:GD_ROW + 1, gd.at(x * gd.ny + y)], faces)
    gram_ref[...] = gram_of(left, right_high, right_low)


def final_kernel(gd, me_ref, mix_ref, *refs):
    parts, (out_ref, both) = [refs[i * gd.n:(i + 1) * gd.n] for i in range(3)], refs[3 * gd.n:]
    me, v = me_ref[0], gd.v
    k = 3 * v
    both[:v, :], both[v:, :] = split(mix_ref[...])
    high, pair = both[:v, :k], both[:, :k]

    def column(i, _):
        at = lanes_of(gd, i)
        value = mix(high, pair, [jnp.concatenate([m[:, at] for m in messages], axis=1) for messages in parts])
        values = [value[:, gd.at(s)] for s in range(gd.n)]
        for q in range(gd.n):
            out_ref[pl.ds(i * gd.n + q, v, stride=gd.blocks), :] = gather(gd, me, v, values, q)
        return 0

    lax.fori_loop(0, gd.blocks // gd.n, column, 0, unroll=3)


def call(kernel, outs, args, scratch=(), flops=1 << 20, vmem=16, scalars=0, free=0):
    vmem_spec = pl.BlockSpec(memory_space=pltpu.VMEM)
    specs = ([pl.BlockSpec(memory_space=pltpu.SMEM)] * scalars + [pl.BlockSpec(memory_space=pl.ANY)] * free
             + [vmem_spec] * (len(args) - scalars - free))
    results = pl.pallas_call(
        kernel,
        out_shape=[jax.ShapeDtypeStruct(s, F32) for s in outs],
        in_specs=specs,
        out_specs=[vmem_spec] * len(outs),
        scratch_shapes=[d if s is None else pltpu.VMEM(s, d) for s, d in scratch],
        compiler_params=pltpu.CompilerParams(vmem_limit_bytes=vmem << 20),
        cost_estimate=pl.CostEstimate(flops=flops, bytes_accessed=1 << 20, transcendentals=0),
    )(*args)
    return list(results)


def exchange(faces):
    nx, ny, nz = (lax.axis_size(a) for a in AXES)
    lines = ((("gx", "gz"), [x * nz + z for z in range(nz) for x in range(nx)]),)
    if ny == 2:
        out = [lax.ppermute(faces[0], "gy", [(0, 1), (1, 0)])]
    else:
        out, lines = [], (("gy", list(range(ny))),) + lines
    for (axes, line), low, high in zip(lines, faces[len(out)::2], faces[len(out) + 1::2]):
        out += both_ways(low, high, axes, line)
    return out


def both_ways(low, high, axes, line):
    up = list(zip(line[:-1], line[1:]))
    return [lax.ppermute(high, axes, up), lax.ppermute(low, axes, [(j, i) for i, j in up])]


def swap(messages):
    n = len(messages)
    return messages[:1] + [lax.ppermute(messages[s], "gx", [(i, i ^ s) for i in range(n)]) for s in range(1, n)]


def sum_over(x, axis):
    n = lax.axis_size(axis)
    if n & (n - 1):
        return lax.psum(x, axis)
    if n <= 4:
        parts = [lax.ppermute(x, axis, [(i, i ^ s) for i in range(n)]) for s in range(1, n)]
        return functools.reduce(jnp.add, parts, x)
    step = 1
    while step < n:
        x = x + lax.ppermute(x, axis, [(i, i ^ step) for i in range(n)])
        step *= 2
    return x


def total(x, later, move):
    n = lax.axis_size("gy")
    me = lax.axis_index("gy")
    half = x.shape[0] // 2
    pair = [(0, 1), (1, 0)]
    piece = lambda k: lax.dynamic_slice_in_dim(x, k * half, half, 0)
    if n == 2:
        mine = piece(me) + lax.ppermute(piece(1 - me), "gy", pair)
    else:
        mine = sum_over(x, "gy")
    mine = sum_over(mine, "gx")
    mine, later = lax.optimization_barrier((mine, later))
    moved = move(later)
    mine = sum_over(mine, "gz")
    if n != 2:
        return mine, moved
    theirs = lax.ppermute(mine, "gy", pair)
    order = [jnp.concatenate(p, 0) for p in ((mine, theirs), (theirs, mine))]
    return jnp.where(me == 0, *order), moved


def local(start_block, stiff_field, shift_field, mass_field):
    n = lax.axis_size("gx")
    gd = Grid(start_block.shape, n, lax.axis_size("gy"))
    v, nz, lanes = gd.v, gd.nz, gd.lanes
    count = stiff_field.size * gd.c
    for axis in AXES:
        count *= lax.axis_size(axis)
    scale = 1.0 / count
    rows = gd.nx * gd.ny
    me = jnp.stack([lax.axis_index("gx"), lax.axis_index("gy")]).astype(jnp.int32)
    fields = [f.reshape(rows, nz) for f in (stiff_field, shift_field, mass_field)]
    native = start_block.reshape(v * gd.blocks, nz)
    faces = [(v, gd.yface)] * gd.ysides + [(v, gd.zface)] * 2
    tall = [(v + 8, gd.yface)] * gd.ysides + [(v + 8, gd.zface)] * 2
    full, square = (v, lanes), (v, v)
    messages = [(v, gd.message)] * n
    part = functools.partial

    *sent, kept = call(part(send_kernel, gd), messages + tall + [(3 * rows, nz)], [me, native] + fields,
                       [((v * gd.blocks, nz), F32), (None, pltpu.SemaphoreType.DMA((4,)))], scalars=1, free=4)
    received = swap(sent[:n])
    yfaces, (zlo, zhi) = sent[n:-2], sent[-2:]
    line = list(range(lax.axis_size("gz")))
    beside = (exchange(yfaces + [zlo, zhi])[:1] if gd.ysides == 1
              else both_ways(*yfaces, "gy", list(range(lax.axis_size("gy")))))
    beside += [zlo, zhi] + both_ways(zhi, zlo, "gz", line)
    around = call(part(halo_kernel, gd), [(v + 8, gd.columns * nz)] * n, [me] + beside + [kept], scalars=1)
    around = swap(around)
    sm, coef, *halo_s = call(part(receive_kernel, gd), [full, (8, rows * nz)] + tall,
                             [me] + received + around, scalars=1)
    gram_scratch = lambda n: [((2 * v, lanes), BF16), ((n * v, lanes), BF16), ((n * v, lanes), BF16)]
    ks, gram0, *faces_u = call(part(image_kernel, gd), [full, (v, 2 * v)] + faces,
                               [me, sm, coef] + halo_s, gram_scratch(2), flops=1 << 32, scalars=1)
    gram0, halo_u = total(gram0, faces_u, exchange)
    coef0, theta0 = call(part(dense0_kernel, scale), [(v, 2 * v), square], [gram0], flops=1 << 31)

    r0, kr0, gram1, *rest = call(part(residual_kernel, gd, False, 1),
                                 [full, full, (v, 4 * v)] + messages + faces + faces,
                                 [me, coef0, coef, ks, sm] + halo_u + halo_s,
                                 [((2 * v, 2 * v), BF16)] + gram_scratch(4), flops=1 << 33, vmem=26, scalars=1)
    r0_sent, halo_r, faces_b = rest[:n], rest[n:n + len(faces)], rest[n + len(faces):]

    def move(a):
        moved = swap(a[0])
        return moved, exchange(a[1])

    gram1, (r0_moved, halo_b) = total(gram1, (r0_sent, faces_b), move)
    coef1, theta1 = call(part(dense1_kernel, scale), [(v, 4 * v), square], [gram1, coef0, theta0],
                         flops=1 << 33)

    gram2, *r1_sent = call(part(residual_kernel, gd, True, 2), [(v, 6 * v)] + messages,
                           [me, coef1, coef, ks, kr0, sm, r0] + halo_u + halo_b + halo_s + halo_r,
                           [((2 * v, 4 * v), BF16)] + gram_scratch(6) + [(full, F32)] + [(f, F32) for f in faces],
                           flops=1 << 33, vmem=32, scalars=1)
    gram2, r1_moved = total(gram2, r1_sent, swap)
    (prev,) = call(part(previous_kernel, scale), [(v, 4 * v)], [gram1, coef1])
    coef2, theta2 = call(part(dense2_kernel, scale), [(v, 4 * v), square], [gram2, prev, coef1, theta1],
                         flops=1 << 33)
    (modes,) = call(part(final_kernel, gd), [(v * gd.blocks, nz)],
                    [me, coef2] + sent[:n] + r0_moved + r1_moved, [((2 * v, 4 * v), BF16)], scalars=1)
    return modes.reshape(start_block.shape), theta2


def solution(mesh):
    grid = P("gx", "gy", "gz")
    block = P(None, None, "gx", "gy", "gz")
    return jax.shard_map(local, mesh=mesh, in_specs=(block, grid, grid, grid), out_specs=(block, P()), check_vma=False)
```
